32 devices in a mesh: design: 2 (over x), blk: 16 (over z, y, core).
Axes of the slice: x: 2, y: 2, z: 4, core: 2. Of those that a mesh axis runs over, the one named last changes fastest.
Arguments:
- right_side: float32 [6, 256, 1024], P(None, ('design', 'blk')), parts along dimension 1, may hold values from -6 to 6
- adjoint_start: float32 [6, 256, 1024], P(None, ('design', 'blk')), parts along dimension 1, may hold values from -3 to 3
- diag_inverse: float32 [6, 6, 256, 1024], P(None, None, ('design', 'blk')), parts along dimension 2
- face_jacobian: bfloat16 [4, 6, 6, 256, 1024], P(None, None, None, ('design', 'blk')), parts along dimension 3, may hold values from -0.25 to 0.25
- receptor_cell: int32 [32, 16, 16], P(('design', 'blk')), parts along dimension 0, may hold values from 0 to 8191
- donor_cell: int32 [32, 16, 4, 16], P(('design', 'blk')), parts along dimension 0, may hold values from 0 to 8191
- donor_weight: float32 [32, 16, 4, 16], P(('design', 'blk')), parts along dimension 0, may hold values from 0 to 1, as said below
- live_count: int32 [32, 16], P(('design', 'blk')), parts along dimension 0, may hold values from 0 to 16, as said below
Outputs:
- adjoint: float32 [6, 256, 1024], P(None, ('design', 'blk')), parts along dimension 1
- correction_norms: float32 [4], P('design'), parts along dimension 0
The draws below stay inside these ranges and needn't reach their ends.
There are 2 independent parts, one for each index of `design`. The reference program is written for one: setup_inputs(seed, part) draws one part's arguments, and reference() takes and returns one part's arrays. A program takes and returns all parts, laid end to end along the dimension named above; each array names one. Nothing has to cross between parts.
Inputs may be any that keep to these rules, and one draw needn't show every extreme that they name: live_count[s, d] counts the leading live slots of list (s, d); in every draw some partition d has 16 live slots from every source s. `donor_weight`: the four weights of each slot are positive and sum to 1.
All inputs are finite; a program needn't handle non-finite values.
Results may differ from the reference program's by a relative error of at most 0.0003.
Values sent between devices are 32-bit elements; how exact they have to be, the bound alone decides.
A program may use at most 64 MiB of HBM per device.

```python
import jax
import jax.numpy as jnp
from jax import lax

NVAR = 6
CJ = 1024
SLOTS = 16
SWEEPS = 2
NB = 16
NI = 128
CELLS_DEV = 8192


def draw_diag_inverse(key, part):
    first, second = jax.random.split(key, 2)
    diagonal = jax.random.uniform(first, (1, 1, NI, CJ), jnp.float32, 0.5, 1.0)
    noise = 0.12 * jax.random.normal(second, (NVAR, NVAR, NI, CJ), jnp.float32)
    identity = jnp.eye(NVAR, dtype=jnp.float32)[:, :, None, None]
    return (identity * diagonal + noise).astype(jnp.float32)


def draw_donor_weight(key, part):
    inner = jax.random.fold_in(key, 29)
    raw = jax.random.uniform(inner, (NB, NB, 4, SLOTS), jnp.float32, 0.05, 0.5)
    total = jnp.sum(raw, axis=2, keepdims=True)
    return (raw / total).astype(jnp.float32)


def draw_live_count(key, part):
    first, second, third = jax.random.split(jax.random.fold_in(key, 17), 3)
    ceiling = jax.random.randint(first, (1, NB), SLOTS // 4, SLOTS + 1)
    base = jax.random.randint(second, (NB, NB), 0, SLOTS + 1)
    full_dest = jax.random.randint(third, (), 0, NB)
    dest = jnp.arange(NB, dtype=jnp.int32)[None, :]
    return jnp.where(dest == full_dest, SLOTS, jnp.minimum(base, ceiling)).astype(jnp.int32)


def touch_ends(drawn, rng, least, high):
    index_at = [jax.random.randint(jax.random.fold_in(rng, axis), (), 0, length) for axis, length in enumerate(drawn.shape)]
    main_axis = drawn.shape.index(max(drawn.shape))
    beside = index_at[:main_axis] + [(index_at[main_axis] + 1) % drawn.shape[main_axis]] + index_at[main_axis + 1:]
    return drawn.at[tuple(index_at)].set(least).at[tuple(beside)].set(high)


def shard_levels(stream_key, extent, pieces, least, high):
    def one(axis_at, shards_of):
        heights = jax.random.uniform(jax.random.fold_in(jax.random.fold_in(stream_key, 6), axis_at), (shards_of,), jnp.float32, least / len(pieces), high / len(pieces))
        return jnp.repeat(jnp.exp(heights), extent[axis_at] // shards_of).reshape((-1,) + (1,) * (len(extent) - axis_at - 1))

    factor_of = one(*pieces[0])
    for cut in pieces[1:]:
        factor_of = factor_of * one(*cut)
    return factor_of


def bell_draw(own_key, dims, width, most, shards=(), held_as=jnp.bfloat16):
    result = width * jax.random.normal(own_key, dims, jnp.float32)
    if shards:
        result = result * shard_levels(own_key, dims, shards, -0.22, 0.18)
    return jnp.clip(result, -most, most).astype(held_as)


def setup_inputs(seed: int = 0, part: int = 0) -> dict:
    key_of = jax.random.split(jax.random.key(seed), 9)
    part_keys = jax.random.split(jax.random.fold_in(key_of[8], part), 9)
    right_side = bell_draw(part_keys[0], (NVAR, NI, CJ), 1.0, 6.0, ((1, 16),), jnp.float32)
    adjoint_start = bell_draw(part_keys[1], (NVAR, NI, CJ), 0.5, 3.0, ((1, 16),), jnp.float32)
    diag_inverse = draw_diag_inverse(jax.random.fold_in(jax.random.fold_in(key_of[8], part), 71), part)
    face_jacobian = bell_draw(part_keys[3], (4, NVAR, NVAR, NI, CJ), 0.04, 0.25, ((3, 16),))
    receptor_cell = touch_ends(jax.random.randint(part_keys[4], (NB, NB, SLOTS), 0, CELLS_DEV), jax.random.fold_in(part_keys[4], 1), 0, CELLS_DEV - 1).astype(jnp.int32)
    donor_cell = touch_ends(jax.random.randint(part_keys[5], (NB, NB, 4, SLOTS), 0, CELLS_DEV), jax.random.fold_in(part_keys[5], 1), 0, CELLS_DEV - 1).astype(jnp.int32)
    donor_weight = draw_donor_weight(jax.random.fold_in(jax.random.fold_in(key_of[8], part), 71), part)
    live_count = draw_live_count(jax.random.fold_in(jax.random.fold_in(key_of[8], part), 71), part)
    return dict(right_side=right_side, adjoint_start=adjoint_start, diag_inverse=diag_inverse, face_jacobian=face_jacobian, receptor_cell=receptor_cell, donor_cell=donor_cell, donor_weight=donor_weight, live_count=live_count)


def transpose_interp(flat_psi, receptor_cell, donor_cell, donor_weight, live_count):
    parts = receptor_cell.shape[0]
    slots = receptor_cell.shape[2]
    cells = flat_psi.shape[1] // parts
    source_base = (jnp.arange(parts, dtype=jnp.int32) * cells).astype(jnp.int32)
    sources = source_base[:, None, None] + receptor_cell
    live = (jnp.arange(slots, dtype=jnp.int32)[None, None, :] < live_count[:, :, None]).astype(jnp.float32)
    values = flat_psi[:, sources] * live[None]
    terms = values[:, :, :, None, :] * donor_weight[None]
    targets = source_base[None, :, None, None] + donor_cell
    spread = jnp.zeros(flat_psi.shape, jnp.float32)
    return spread.at[:, targets.reshape(-1)].add(terms.reshape(flat_psi.shape[0], -1))

def neighbours(psi):
    padded = jnp.pad(psi, ((0, 0), (1, 1), (1, 1)))
    return (padded[:, :-2, 1:-1], padded[:, 2:, 1:-1], padded[:, 1:-1, :-2], padded[:, 1:-1, 2:])

def reference(right_side, adjoint_start, diag_inverse, face_jacobian, receptor_cell, donor_cell, donor_weight, live_count):
    nvar, rows, cols = right_side.shape
    rhs_sq = jnp.sum(right_side * right_side)
    psi = adjoint_start
    norms = []
    for sweep in range(SWEEPS):
        spread = transpose_interp(psi.reshape(nvar, rows * cols), receptor_cell, donor_cell, donor_weight, live_count)
        coupled = jnp.zeros(psi.shape, jnp.float32)
        sides = neighbours(psi)
        for face in range(4):
            coupled = coupled + jnp.einsum('abij,bij->aij', face_jacobian[face].astype(jnp.float32), sides[face], precision=lax.Precision.HIGHEST)
        source = right_side - coupled + spread.reshape(psi.shape)
        new = jnp.einsum('abij,bij->aij', diag_inverse, source, precision=lax.Precision.HIGHEST)
        change = new - psi
        norms.append(jnp.sqrt(jnp.sum(change * change) / (rhs_sq + 1e-06)))
        psi = new
    return (psi, jnp.stack(norms).astype(jnp.float32))
```

```python
import functools

import jax
import jax.numpy as jnp
from jax import lax
from jax.experimental import pallas as pl
from jax.experimental.pallas import tpu as pltpu
from jax.sharding import PartitionSpec as P

SWEEPS = 2
LANES = 128
MESH = pl.DeviceIdType.MESH
F32 = jnp.float32
BF16 = jnp.bfloat16


def two_pieces(x):
    high = x.astype(BF16)
    low = (x - high.astype(F32)).astype(BF16)
    return high, low


def wait_bytes(ref, sem):
    pltpu.make_async_copy(ref, ref, sem).wait()


def kernel(
    n,
    live_s,
    rhs_h,
    psi_h,
    dinv_h,
    jac_h,
    rec_h,
    don_h,
    wgt_h,
    out_ref,
    norm_s,
    rhs,
    psi0,
    psi1,
    dinv,
    jac,
    rec,
    don,
    wgt,
    acc,
    near,
    recpad,
    stage,
    stage_in,
    vsend,
    vrecv,
    hsend,
    hrecv,
    nsend,
    nrecv,
    pick_hot,
    pick_block,
    add_hot,
    add_block,
    lhs,
    weights,
    local_sem,
    stage_sem,
    v_sem,
    h_sem,
    n_sem,
):
    nvar, rows, cols = psi0.shape
    slots = rec.shape[1]
    donors = don.shape[1]
    lists = n * slots
    per = LANES // slots
    tiles = lists // LANES
    width = pick_hot.shape[0]
    strips = cols // width
    blocks = rows * strips
    full = nvar * blocks
    me = lax.axis_index("blk")
    design = lax.axis_index("design")

    barrier = pltpu.get_barrier_semaphore()

    def greet(j, carry):
        pl.semaphore_signal(
            barrier, inc=1, device_id=(design, lax.rem(me + j, n)), device_id_type=MESH
        )
        return carry

    lax.fori_loop(1, n, greet, 0)

    loads = []
    for k, (src, dst) in enumerate(
        (
            (psi_h, psi0),
            (rec_h.at[0], rec),
            (don_h.at[0], don),
            (wgt_h.at[0], wgt),
            (jac_h, jac),
            (rhs_h, rhs),
            (dinv_h, dinv),
        )
    ):
        copy = pltpu.make_async_copy(src, dst, local_sem.at[k])
        copy.start()
        loads.append(copy)

    def split_cell(row):
        i = jnp.floor((row + 0.5) * (1.0 / cols))
        j = row - i * cols
        q = jnp.floor((j + 0.5) * (1.0 / width))
        return (q * rows + i).astype(jnp.int32), (j - q * width).astype(jnp.int32)

    def to_all(source_of, dest_ref, send_sem, recv_sem):
        def send(j, carry):
            dest = lax.rem(me + j, n)
            pltpu.make_async_remote_copy(
                src_ref=source_of(dest),
                dst_ref=dest_ref.at[me],
                send_sem=send_sem,
                recv_sem=recv_sem,
                device_id=(design, dest),
                device_id_type=MESH,
            ).start()
            return carry

        lax.fori_loop(1, n, send, 0)

    def halo_copies(sweep):
        below = lax.rem(me + n - 1, n)
        above = lax.rem(me + 1, n)
        return [
            pltpu.make_async_remote_copy(
                src_ref=hsend.at[sweep, side],
                dst_ref=hrecv.at[sweep, side],
                send_sem=h_sem.at[sweep, side, 0],
                recv_sem=h_sem.at[sweep, side, 1],
                device_id=(design, target),
                device_id_type=MESH,
            )
            for side, target in ((0, above), (1, below))
        ]

    def assemble(tile_of):
        parts = []
        for h in range(tiles):
            total = None
            for g in range(per):
                tile = tile_of(h * per + g)
                if g:
                    tile = pltpu.roll(tile, g * slots, 1)
                total = tile if total is None else total + tile
            parts.append(total)
        return parts

    def put_halo(sweep, psi):
        hsend[sweep, 0] = psi[:, rows - 1, :]
        hsend[sweep, 1] = psi[:, 0, :]

    def pick(sweep, psi):
        x = jnp.concatenate(
            [psi[a, :, q * width : (q + 1) * width] for a in range(nvar) for q in range(strips)],
            axis=0,
        )
        high, low = two_pieces(x)
        got = jnp.dot(
            jnp.concatenate([high, low], axis=0), pick_hot[...], preferred_element_type=F32
        )
        got = (got[:full] + got[full:]).reshape(nvar, blocks, lists)
        got = jnp.sum(got * pick_block[...][None], axis=1)
        for h in range(tiles):
            vsend[sweep, h, 0:nvar, :] = got[:, h * LANES : (h + 1) * LANES]

    stage[...] = jnp.zeros(stage.shape, F32)
    recpad[...] = jnp.zeros(recpad.shape, F32)
    vsend[...] = jnp.zeros(vsend.shape, F32)
    loads[1].wait()
    recpad[:, 0:slots] = rec[...].astype(F32)
    loads[2].wait()
    loads[3].wait()
    slot_id = lax.broadcasted_iota(jnp.int32, (donors, slots), 1)

    def fill(d):
        stage[d, 0:donors, 0:slots] = don[d].astype(F32)
        stage[d, donors : 2 * donors, 0:slots] = jnp.where(slot_id < live_s[0, d], wgt[d], 0.0)

    for d in range(n):
        fill(d)
    loads[0].wait()
    put_halo(0, psi0)

    pl.semaphore_wait(barrier, n - 1)
    halos = [halo_copies(s) for s in range(SWEEPS)]
    to_all(lambda dest: stage.at[dest], stage_in, stage_sem.at[0], stage_sem.at[1])
    for copy in halos[0]:
        copy.start()

    cells = jnp.concatenate(assemble(lambda d: recpad[d : d + 1, :]), axis=1)
    upper, lower = split_cell(cells)
    pick_hot[...] = (
        lax.broadcasted_iota(jnp.int32, (width, lists), 0) == lower
    ).astype(F32).astype(BF16)
    pick_block[...] = (lax.broadcasted_iota(jnp.int32, (blocks, lists), 0) == upper).astype(F32)
    pick(0, psi0)
    to_all(lambda dest: vsend.at[0, dest // per], vrecv.at[0], v_sem.at[0, 0], v_sem.at[0, 1])

    lane_of = lax.broadcasted_iota(jnp.int32, (8, LANES), 1)
    my_group = lax.rem(me, per)
    mine = (lane_of >= my_group * slots) & (lane_of < (my_group + 1) * slots)
    back = lax.rem((per - my_group) * slots, LANES)

    def couple(psi, sweep, faces, first):
        def chunk(c, carry):
            at = pl.ds(pl.multiple_of(c * LANES, LANES), LANES)
            values = [[near[f % 2, b, :, at] for b in range(nvar)] for f in faces]
            for a in range(nvar):
                total = rhs[a, :, at] if first else acc[a, :, at]
                for k, f in enumerate(faces):
                    for b in range(nvar):
                        total = total - jac[f, a, b, :, at].astype(F32) * values[k][b]
                acc[a, :, at] = total
            return carry

        lax.fori_loop(0, cols // LANES, chunk, 0)

    col_id = lax.broadcasted_iota(jnp.int32, (rows, cols), 1)
    row_id = lax.broadcasted_iota(jnp.int32, (rows, cols), 0)

    def sides(psi, sweep):
        for b in range(nvar):
            x = psi[b]
            near[0, b] = jnp.where(col_id == 0, 0.0, pltpu.roll(x, 1, 1))
            near[1, b] = jnp.where(col_id == cols - 1, 0.0, pltpu.roll(x, cols - 1, 1))

    def ends(psi, sweep):
        for copy in halos[sweep]:
            copy.wait_recv()
        for b in range(nvar):
            x = psi[b]
            low = jnp.where(me > 0, hrecv[sweep, 0, b : b + 1, :], 0.0)
            high = jnp.where(me < n - 1, hrecv[sweep, 1, b : b + 1, :], 0.0)
            near[0, b] = jnp.where(row_id == 0, low, pltpu.roll(x, 1, 0))
            near[1, b] = jnp.where(row_id == rows - 1, high, pltpu.roll(x, rows - 1, 0))

    def prepare_adds():
        wait_bytes(stage_in.at[pl.ds(0, n - 1)], stage_sem.at[1])
        stage_in[me] = stage[me]
        packed = jnp.concatenate(assemble(lambda s: stage_in[s]), axis=1)
        weights[...] = packed[donors : 2 * donors]
        for m in range(donors):
            upper, lower = split_cell(packed[m : m + 1])
            at = slice(m * lists, (m + 1) * lists)
            add_hot[:, at] = (
                lax.broadcasted_iota(jnp.int32, (width, lists), 0) == lower
            ).astype(F32).astype(BF16)
            add_block[m] = (
                lax.broadcasted_iota(jnp.int32, (blocks, lists), 0) == upper
            ).astype(F32)

    def add_donors(sweep):
        wait_bytes(vrecv.at[sweep, pl.ds(0, n - 1)], v_sem.at[sweep, 1])
        vrecv[sweep, me] = vsend[sweep, me // per]
        parts = assemble(lambda s: jnp.where(mine, vrecv[sweep, s], 0.0))
        values = jnp.concatenate([pltpu.roll(part, back, 1) for part in parts], axis=1)
        for m in range(donors):
            terms = values * weights[m : m + 1, :]
            pieces = two_pieces(terms)
            for k, piece in enumerate(pieces):
                piece = piece.astype(F32)
                for a in range(nvar):
                    at = k * full + a * blocks
                    lhs[at : at + blocks, m * lists : (m + 1) * lists] = (
                        add_block[m] * piece[a : a + 1, :]
                    ).astype(BF16)
        got = lax.dot_general(
            lhs[...], add_hot[...], (((1,), (1,)), ((), ())), preferred_element_type=F32
        )
        got = got[:full] + got[full:]
        for a in range(nvar):
            for q in range(strips):
                at = a * blocks + q * rows
                col = slice(q * width, (q + 1) * width)
                acc[a, :, col] = acc[a, :, col] + got[at : at + rows]

    def finish(psi, new):
        def chunk(c, total):
            at = pl.ds(pl.multiple_of(c * LANES, LANES), LANES)
            source = [acc[b, :, at] for b in range(nvar)]
            for a in range(nvar):
                value = dinv[a, 0, :, at] * source[0]
                for b in range(1, nvar):
                    value = value + dinv[a, b, :, at] * source[b]
                change = value - psi[a, :, at]
                total = total + change * change
                new[a, :, at] = value
            return total

        return lax.fori_loop(0, cols // LANES, chunk, jnp.zeros((rows, LANES), F32))

    sums = []
    psi = psi0
    for sweep in range(SWEEPS):
        new = out_ref if sweep == SWEEPS - 1 else psi1
        sides(psi, sweep)
        if sweep == 0:
            loads[4].wait()
            loads[5].wait()
        couple(psi, sweep, (2, 3), True)
        if sweep == 0:
            def square(c, total):
                at = pl.ds(pl.multiple_of(c * LANES, LANES), LANES)
                for a in range(nvar):
                    value = rhs[a, :, at]
                    total = total + value * value
                return total

            sums.append(
                lax.fori_loop(0, cols // LANES, square, jnp.zeros((rows, LANES), F32))
            )
            prepare_adds()
        ends(psi, sweep)
        couple(psi, sweep, (0, 1), False)
        add_donors(sweep)
        if sweep == 0:
            loads[6].wait()
        sums.append(finish(psi, new))
        psi = new
        if sweep + 1 < SWEEPS:
            pick(sweep + 1, psi)
            to_all(
                lambda dest: vsend.at[sweep + 1, dest // per],
                vrecv.at[sweep + 1],
                v_sem.at[sweep + 1, 0],
                v_sem.at[sweep + 1, 1],
            )
            put_halo(sweep + 1, psi)
            for copy in halos[sweep + 1]:
                copy.start()

    lines = [jnp.sum(s, axis=0, keepdims=True) for s in sums]
    lines.append(jnp.zeros((8 - len(lines), LANES), F32))
    nsend[...] = jnp.concatenate(lines, axis=0)
    to_all(lambda dest: nsend, nrecv, n_sem.at[0], n_sem.at[1])
    wait_bytes(stage_in.at[pl.ds(0, n - 1)], stage_sem.at[0])
    for sweep in range(SWEEPS):
        wait_bytes(vrecv.at[sweep, pl.ds(0, n - 1)], v_sem.at[sweep, 0])
        for copy in halos[sweep]:
            copy.wait_send()
    wait_bytes(nrecv.at[pl.ds(0, n - 1)], n_sem.at[1])
    nrecv[me] = nsend[...]
    total = nrecv[0]
    for s in range(1, n):
        total = total + nrecv[s]
    total = jnp.sum(total, axis=1, keepdims=True)
    result = jnp.sqrt(total[1 : 1 + SWEEPS] / (total[0:1] + 1e-6))
    for k in range(SWEEPS):
        norm_s[k] = result[k, 0]
    wait_bytes(nrecv.at[pl.ds(0, n - 1)], n_sem.at[0])


def body(n, right_side, adjoint_start, diag_inverse, face_jacobian, receptor, donor, weight, live):
    nvar, rows, cols = right_side.shape
    slots = receptor.shape[2]
    donors = donor.shape[2]
    lists = n * slots
    width = min(256, cols)
    blocks = rows * (cols // width)
    tiles = lists // LANES
    any_space = pl.BlockSpec(memory_space=pl.ANY)
    field = pltpu.VMEM((nvar, rows, cols), F32)
    adjoint, norms = pl.pallas_call(
        functools.partial(kernel, n),
        out_shape=(
            jax.ShapeDtypeStruct((nvar, rows, cols), F32),
            jax.ShapeDtypeStruct((SWEEPS,), F32),
        ),
        in_specs=[pl.BlockSpec(memory_space=pltpu.SMEM)] + [any_space] * 7,
        out_specs=(
            pl.BlockSpec(memory_space=pltpu.VMEM),
            pl.BlockSpec(memory_space=pltpu.SMEM),
        ),
        scratch_shapes=[
            field,
            field,
            field,
            pltpu.VMEM(diag_inverse.shape, F32),
            pltpu.VMEM(face_jacobian.shape, face_jacobian.dtype),
            pltpu.VMEM((n, slots), jnp.int32),
            pltpu.VMEM((n, donors, slots), jnp.int32),
            pltpu.VMEM((n, donors, slots), F32),
            field,
            pltpu.VMEM((2, nvar, rows, cols), F32),
            pltpu.VMEM((n, LANES), F32),
            pltpu.VMEM((n, 8, LANES), F32),
            pltpu.VMEM((n, 8, LANES), F32),
            pltpu.VMEM((SWEEPS, tiles, 8, LANES), F32),
            pltpu.VMEM((SWEEPS, n, 8, LANES), F32),
            pltpu.VMEM((SWEEPS, 2, nvar, cols), F32),
            pltpu.VMEM((SWEEPS, 2, nvar, cols), F32),
            pltpu.VMEM((8, LANES), F32),
            pltpu.VMEM((n, 8, LANES), F32),
            pltpu.VMEM((width, lists), BF16),
            pltpu.VMEM((blocks, lists), F32),
            pltpu.VMEM((width, donors * lists), BF16),
            pltpu.VMEM((donors, blocks, lists), F32),
            pltpu.VMEM((2 * nvar * blocks, donors * lists), BF16),
            pltpu.VMEM((donors, lists), F32),
            pltpu.SemaphoreType.DMA((7,)),
            pltpu.SemaphoreType.DMA((2,)),
            pltpu.SemaphoreType.DMA((SWEEPS, 2)),
            pltpu.SemaphoreType.DMA((SWEEPS, 2, 2)),
            pltpu.SemaphoreType.DMA((2,)),
        ],
        compiler_params=pltpu.CompilerParams(
            collective_id=0, has_side_effects=True, vmem_limit_bytes=60 * 1024 * 1024
        ),
    )(live, right_side, adjoint_start, diag_inverse, face_jacobian, receptor, donor, weight)
    return adjoint, norms


def solution(mesh):
    return jax.shard_map(
        functools.partial(body, mesh.shape["blk"]),
        mesh=mesh,
        in_specs=(
            P(None, ("design", "blk"), None),
            P(None, ("design", "blk"), None),
            P(None, None, ("design", "blk"), None),
            P(None, None, None, ("design", "blk"), None),
            P(("design", "blk"), None, None),
            P(("design", "blk"), None, None, None),
            P(("design", "blk"), None, None, None),
            P(("design", "blk"), None),
        ),
        out_specs=(P(None, ("design", "blk"), None), P("design")),
        check_vma=False,
    )
```

```python
import functools

import jax
import jax.numpy as jnp
from jax import lax
from jax.experimental import pallas as pl
from jax.experimental.pallas import tpu as pltpu
from jax.sharding import PartitionSpec as P

SWEEPS = 2
LANES = 128
MESH = pl.DeviceIdType.MESH
F32 = jnp.float32
BF16 = jnp.bfloat16


def two_pieces(x):
    high = x.astype(BF16)
    low = (x - high.astype(F32)).astype(BF16)
    return high, low


def swap_groups(x, slots):
    height, lanes = x.shape
    row = lax.broadcasted_iota(jnp.int32, x.shape, 0)
    lane = lax.broadcasted_iota(jnp.int32, x.shape, 1)
    bit = 1
    while bit < height:
        step = bit * slots
        differ = ((row * slots) ^ lane) & step
        up = pltpu.roll(pltpu.roll(x, bit, 0), lanes - step, 1)
        down = pltpu.roll(pltpu.roll(x, height - bit, 0), step, 1)
        x = jnp.where(differ == 0, x, jnp.where((row & bit) != 0, up, down))
        bit *= 2
    return x


def wait_bytes(ref, sem):
    pltpu.make_async_copy(ref, ref, sem).wait()


def kernel(
    n,
    rhs_h,
    psi_h,
    dinv_h,
    jac_h,
    rec_h,
    don_h,
    wgt_h,
    live_h,
    out_ref,
    total_ref,
    rhs,
    psi0,
    psi1,
    dinv,
    jac,
    rec,
    don,
    wgt,
    live_s,
    acc,
    near,
    recpad,
    stage,
    first_out,
    first_in,
    later_out,
    later_in,
    hsend,
    hrecv,
    nsend,
    nrecv,
    pick_hot,
    pick_block,
    add_hot,
    add_block,
    lhs,
    weights,
    local_sem,
    v_sem,
    h_sem,
    n_sem,
):
    nvar, rows, cols = psi0.shape
    slots = rec.shape[1]
    donors = don.shape[1]
    lists = n * slots
    per = LANES // slots
    tiles = lists // LANES
    width = pick_hot.shape[0]
    strips = cols // width
    blocks = rows * strips
    full = nvar * blocks
    me = lax.axis_index("blk")
    design = lax.axis_index("design")

    barrier = pltpu.get_barrier_semaphore()

    def greet(j, carry):
        pl.semaphore_signal(
            barrier, inc=1, device_id=(design, lax.rem(me + j, n)), device_id_type=MESH
        )
        return carry

    lax.fori_loop(1, n, greet, 0)

    loads = []
    for k, (src, dst) in enumerate(
        (
            (rec_h.at[0], rec),
            (don_h.at[0], don),
            (wgt_h.at[0], wgt),
            (psi_h, psi0),
            (jac_h, jac),
            (rhs_h, rhs),
            (dinv_h, dinv),
            (live_h, live_s),
        )
    ):
        copy = pltpu.make_async_copy(src, dst, local_sem.at[k])
        copy.start()
        loads.append(copy)

    def split_cell(row):
        i = jnp.floor((row + 0.5) * (1.0 / cols))
        j = row - i * cols
        q = jnp.floor((j + 0.5) * (1.0 / width))
        return (q * rows + i).astype(jnp.int32), (j - q * width).astype(jnp.int32)

    def to_all(source_of, dest_ref, send_sem, recv_sem):
        def send(j, carry):
            dest = lax.rem(me + j, n)
            pltpu.make_async_remote_copy(
                src_ref=source_of(dest),
                dst_ref=dest_ref.at[me],
                send_sem=send_sem,
                recv_sem=recv_sem,
                device_id=(design, dest),
                device_id_type=MESH,
            ).start()
            return carry

        lax.fori_loop(1, n, send, 0)

    def halo_copies(sweep):
        below = lax.rem(me + n - 1, n)
        above = lax.rem(me + 1, n)
        return [
            pltpu.make_async_remote_copy(
                src_ref=hsend.at[sweep, side],
                dst_ref=hrecv.at[sweep, side],
                send_sem=h_sem.at[sweep, side, 0],
                recv_sem=h_sem.at[sweep, side, 1],
                device_id=(design, target),
                device_id_type=MESH,
            )
            for side, target in ((0, above), (1, below))
        ]

    def assemble(tile_of):
        parts = []
        for h in range(tiles):
            total = None
            for g in range(per):
                tile = tile_of(h * per + g)
                if g:
                    tile = pltpu.roll(tile, g * slots, 1)
                total = tile if total is None else total + tile
            parts.append(total)
        return parts

    def put_halo(sweep, psi):
        hsend[sweep, 0] = psi[:, rows - 1, :]
        hsend[sweep, 1] = psi[:, 0, :]

    def pick(sweep, psi):
        x = jnp.concatenate(
            [psi[a, :, q * width : (q + 1) * width] for a in range(nvar) for q in range(strips)],
            axis=0,
        )
        high, low = two_pieces(x)
        got = jnp.dot(
            jnp.concatenate([high, low], axis=0), pick_hot[...], preferred_element_type=F32
        )
        got = (got[:full] + got[full:]).reshape(nvar, blocks, lists)
        got = jnp.sum(got * pick_block[...][None], axis=1)
        got = jnp.concatenate([got, jnp.zeros((per - nvar, lists), F32)], axis=0)
        for h in range(tiles):
            packed = swap_groups(got[:, h * LANES : (h + 1) * LANES], slots)
            if sweep == 0:
                first_out[h * per : (h + 1) * per, 1, :] = packed
            else:
                later_out[sweep - 1, h * per : (h + 1) * per, 0, :] = packed

    stage[...] = jnp.zeros(stage.shape, F32)
    recpad[...] = jnp.zeros(recpad.shape, F32)
    loads[0].wait()
    recpad[:, 0:slots] = rec[...].astype(F32)
    cells = jnp.concatenate(assemble(lambda d: recpad[d : d + 1, :]), axis=1)
    upper, lower = split_cell(cells)
    pick_hot[...] = (
        lax.broadcasted_iota(jnp.int32, (width, lists), 0) == lower
    ).astype(F32).astype(BF16)
    pick_block[...] = (lax.broadcasted_iota(jnp.int32, (blocks, lists), 0) == upper).astype(F32)
    loads[1].wait()
    loads[2].wait()
    loads[7].wait()
    slot_id = lax.broadcasted_iota(jnp.int32, (donors, slots), 1)
    for d in range(n):
        stage[d, 0:donors, 0:slots] = don[d].astype(F32)
        stage[d, donors : 2 * donors, 0:slots] = jnp.where(slot_id < live_s[0, d], wgt[d], 0.0)
    for h, part in enumerate(assemble(lambda d: stage[d])):
        first_out[h * per : (h + 1) * per, 0, :] = swap_groups(part, slots)
    loads[3].wait()
    put_halo(0, psi0)
    pick(0, psi0)

    pl.semaphore_wait(barrier, n - 1)
    halos = [halo_copies(s) for s in range(SWEEPS)]
    to_all(lambda dest: first_out.at[dest], first_in, v_sem.at[0, 0], v_sem.at[0, 1])
    for copy in halos[0]:
        copy.start()

    def couple(psi, sweep, faces, first):
        def chunk(c, carry):
            at = pl.ds(pl.multiple_of(c * LANES, LANES), LANES)
            values = [[near[f, b, :, at] for b in range(nvar)] for f in faces]
            for a in range(nvar):
                total = rhs[a, :, at] if first else acc[a, :, at]
                for k, f in enumerate(faces):
                    for b in range(nvar):
                        total = total - jac[f, a, b, :, at].astype(F32) * values[k][b]
                acc[a, :, at] = total
            return carry

        lax.fori_loop(0, cols // LANES, chunk, 0)

    col_id = lax.broadcasted_iota(jnp.int32, (rows, cols), 1)
    row_id = lax.broadcasted_iota(jnp.int32, (rows, cols), 0)

    def sides(psi, sweep):
        for b in range(nvar):
            x = psi[b]
            near[2, b] = jnp.where(col_id == 0, 0.0, pltpu.roll(x, 1, 1))
            near[3, b] = jnp.where(col_id == cols - 1, 0.0, pltpu.roll(x, cols - 1, 1))

    def ends(psi, sweep):
        for copy in halos[sweep]:
            copy.wait_recv()
        for b in range(nvar):
            x = psi[b]
            low = jnp.where(me > 0, hrecv[sweep, 0, b : b + 1, :], 0.0)
            high = jnp.where(me < n - 1, hrecv[sweep, 1, b : b + 1, :], 0.0)
            near[0, b] = jnp.where(row_id == 0, low, pltpu.roll(x, 1, 0))
            near[1, b] = jnp.where(row_id == rows - 1, high, pltpu.roll(x, rows - 1, 0))

    def prepare_adds():
        wait_bytes(first_in.at[pl.ds(0, n - 1)], v_sem.at[0, 1])
        first_in[me] = first_out[me]
        packed = jnp.concatenate(
            [
                swap_groups(first_in[h * per : (h + 1) * per, 0, :], slots)
                for h in range(tiles)
            ],
            axis=1,
        )
        weights[...] = packed[donors : 2 * donors]
        for m in range(donors):
            upper, lower = split_cell(packed[m : m + 1])
            at = slice(m * lists, (m + 1) * lists)
            add_hot[:, at] = (
                lax.broadcasted_iota(jnp.int32, (width, lists), 0) == lower
            ).astype(F32).astype(BF16)
            add_block[m] = (
                lax.broadcasted_iota(jnp.int32, (blocks, lists), 0) == upper
            ).astype(F32)

    def add_donors(sweep):
        if sweep == 0:
            parts = [first_in[h * per : (h + 1) * per, 1, :] for h in range(tiles)]
        else:
            wait_bytes(later_in.at[sweep - 1, pl.ds(0, n - 1)], v_sem.at[sweep, 1])
            later_in[sweep - 1, me] = later_out[sweep - 1, me]
            parts = [
                later_in[sweep - 1, h * per : (h + 1) * per, 0, :] for h in range(tiles)
            ]
        values = jnp.concatenate([swap_groups(part, slots) for part in parts], axis=1)
        for m in range(donors):
            terms = values * weights[m : m + 1, :]
            pieces = two_pieces(terms)
            for k, piece in enumerate(pieces):
                piece = piece.astype(F32)
                for a in range(nvar):
                    at = k * full + a * blocks
                    lhs[at : at + blocks, m * lists : (m + 1) * lists] = (
                        add_block[m] * piece[a : a + 1, :]
                    ).astype(BF16)
        got = lax.dot_general(
            lhs[...], add_hot[...], (((1,), (1,)), ((), ())), preferred_element_type=F32
        )
        got = got[:full] + got[full:]
        for a in range(nvar):
            for q in range(strips):
                at = a * blocks + q * rows
                col = slice(q * width, (q + 1) * width)
                acc[a, :, col] = acc[a, :, col] + got[at : at + rows]

    def finish(psi, new):
        def chunk(c, total):
            at = pl.ds(pl.multiple_of(c * LANES, LANES), LANES)
            source = [acc[b, :, at] for b in range(nvar)]
            for a in range(nvar):
                value = dinv[a, 0, :, at] * source[0]
                for b in range(1, nvar):
                    value = value + dinv[a, b, :, at] * source[b]
                change = value - psi[a, :, at]
                total = total + change * change
                new[a, :, at] = value
            return total

        return lax.fori_loop(0, cols // LANES, chunk, jnp.zeros((rows, LANES), F32))

    sums = []
    psi = psi0
    for sweep in range(SWEEPS):
        new = out_ref if sweep == SWEEPS - 1 else psi1
        sides(psi, sweep)
        if sweep == 0:
            loads[4].wait()
            loads[5].wait()
        couple(psi, sweep, (2, 3), True)
        if sweep == 0:
            def square(c, total):
                at = pl.ds(pl.multiple_of(c * LANES, LANES), LANES)
                for a in range(nvar):
                    value = rhs[a, :, at]
                    total = total + value * value
                return total

            sums.append(
                lax.fori_loop(0, cols // LANES, square, jnp.zeros((rows, LANES), F32))
            )
            prepare_adds()
        ends(psi, sweep)
        couple(psi, sweep, (0, 1), False)
        add_donors(sweep)
        if sweep == 0:
            loads[6].wait()
        sums.append(finish(psi, new))
        psi = new
        if sweep + 1 < SWEEPS:
            pick(sweep + 1, psi)
            to_all(
                lambda dest: later_out.at[sweep, dest],
                later_in.at[sweep],
                v_sem.at[sweep + 1, 0],
                v_sem.at[sweep + 1, 1],
            )
            put_halo(sweep + 1, psi)
            for copy in halos[sweep + 1]:
                copy.start()

    lane = lax.broadcasted_iota(jnp.int32, (1, LANES), 1)
    row = jnp.zeros((1, LANES), F32)
    for q, part in enumerate(sums):
        line = jnp.sum(part, axis=0, keepdims=True)
        line = line + pltpu.roll(line, 64, 1)
        line = line + pltpu.roll(line, 32, 1)
        row = jnp.where((lane >= 32 * q) & (lane < 32 * (q + 1)), line, row)
    nsend[...] = row
    to_all(lambda dest: nsend, nrecv, n_sem.at[0], n_sem.at[1])
    wait_bytes(first_in.at[pl.ds(0, n - 1)], v_sem.at[0, 0])
    for sweep in range(SWEEPS):
        if sweep:
            wait_bytes(later_in.at[sweep - 1, pl.ds(0, n - 1)], v_sem.at[sweep, 0])
        for copy in halos[sweep]:
            copy.wait_send()
    wait_bytes(nrecv.at[pl.ds(0, n - 1)], n_sem.at[1])
    nrecv[me] = nsend[...]
    total = nrecv[0]
    for s in range(1, n):
        total = total + nrecv[s]
    total_ref[...] = total
    wait_bytes(nrecv.at[pl.ds(0, n - 1)], n_sem.at[0])


def close(adjoint_ref, total_ref, out_h, norm_s, sem):
    copy = pltpu.make_async_copy(adjoint_ref, out_h, sem)
    copy.start()
    lane = lax.broadcasted_iota(jnp.int32, (1, LANES), 1)
    total = total_ref[...]
    sums = [
        jnp.sum(
            jnp.where((lane >= 32 * q) & (lane < 32 * (q + 1)), total, 0.0), axis=1, keepdims=True
        )
        for q in range(SWEEPS + 1)
    ]
    for k in range(SWEEPS):
        result = jnp.sqrt(sums[k + 1] / (sums[0] + 1e-6))
        norm_s[k] = result[0, 0]
    copy.wait()


def body(n, right_side, adjoint_start, diag_inverse, face_jacobian, receptor, donor, weight, live):
    nvar, rows, cols = right_side.shape
    slots = receptor.shape[2]
    donors = donor.shape[2]
    lists = n * slots
    width = min(256, cols)
    blocks = rows * (cols // width)
    any_space = pl.BlockSpec(memory_space=pl.ANY)
    field = pltpu.VMEM((nvar, rows, cols), F32)
    placed = [
        pltpu.with_memory_space_constraint(x, pltpu.HBM)
        for x in (
            right_side,
            adjoint_start,
            diag_inverse,
            face_jacobian,
            receptor,
            donor,
            weight,
            live,
        )
    ]
    adjoint, total = pl.pallas_call(
        functools.partial(kernel, n),
        out_shape=(
            jax.ShapeDtypeStruct((nvar, rows, cols), F32),
            jax.ShapeDtypeStruct((1, LANES), F32),
        ),
        in_specs=[pl.BlockSpec(memory_space=pltpu.HBM)] * 8,
        out_specs=(
            pl.BlockSpec(memory_space=pltpu.VMEM),
            pl.BlockSpec(memory_space=pltpu.VMEM),
        ),
        scratch_shapes=[
            field,
            field,
            field,
            pltpu.VMEM(diag_inverse.shape, F32),
            pltpu.VMEM(face_jacobian.shape, face_jacobian.dtype),
            pltpu.VMEM((n, slots), jnp.int32),
            pltpu.VMEM((n, donors, slots), jnp.int32),
            pltpu.VMEM((n, donors, slots), F32),
            pltpu.SMEM((1, n), jnp.int32),
            field,
            pltpu.VMEM((4, nvar, rows, cols), F32),
            pltpu.VMEM((n, LANES), F32),
            pltpu.VMEM((n, 2 * donors, LANES), F32),
            pltpu.VMEM((n, 2, LANES), F32),
            pltpu.VMEM((n, 2, LANES), F32),
            pltpu.VMEM((SWEEPS - 1, n, 1, LANES), F32),
            pltpu.VMEM((SWEEPS - 1, n, 1, LANES), F32),
            pltpu.VMEM((SWEEPS, 2, nvar, cols), F32),
            pltpu.VMEM((SWEEPS, 2, nvar, cols), F32),
            pltpu.VMEM((1, LANES), F32),
            pltpu.VMEM((n, 1, LANES), F32),
            pltpu.VMEM((width, lists), BF16),
            pltpu.VMEM((blocks, lists), F32),
            pltpu.VMEM((width, donors * lists), BF16),
            pltpu.VMEM((donors, blocks, lists), F32),
            pltpu.VMEM((2 * nvar * blocks, donors * lists), BF16),
            pltpu.VMEM((donors, lists), F32),
            pltpu.SemaphoreType.DMA((8,)),
            pltpu.SemaphoreType.DMA((SWEEPS, 2)),
            pltpu.SemaphoreType.DMA((SWEEPS, 2, 2)),
            pltpu.SemaphoreType.DMA((2,)),
        ],
        compiler_params=pltpu.CompilerParams(
            collective_id=0, has_side_effects=True, vmem_limit_bytes=36 * 1024 * 1024
        ),
    )(*placed)
    return pl.pallas_call(
        close,
        out_shape=(
            jax.ShapeDtypeStruct((nvar, rows, cols), F32),
            jax.ShapeDtypeStruct((SWEEPS,), F32),
        ),
        in_specs=[pl.BlockSpec(memory_space=pltpu.VMEM)] * 2,
        out_specs=(any_space, pl.BlockSpec(memory_space=pltpu.SMEM)),
        scratch_shapes=[pltpu.SemaphoreType.DMA],
        compiler_params=pltpu.CompilerParams(vmem_limit_bytes=8 * 1024 * 1024),
    )(adjoint, total)


def solution(mesh):
    return jax.shard_map(
        functools.partial(body, mesh.shape["blk"]),
        mesh=mesh,
        in_specs=(
            P(None, ("design", "blk"), None),
            P(None, ("design", "blk"), None),
            P(None, None, ("design", "blk"), None),
            P(None, None, None, ("design", "blk"), None),
            P(("design", "blk"), None, None),
            P(("design", "blk"), None, None, None),
            P(("design", "blk"), None, None, None),
            P(("design", "blk"), None),
        ),
        out_specs=(P(None, ("design", "blk"), None), P("design")),
        check_vma=False,
    )
```

```python
import functools

import jax
import jax.numpy as jnp
from jax import lax
from jax.experimental import pallas as pl
from jax.experimental.pallas import tpu as pltpu
from jax.sharding import PartitionSpec as P

SWEEPS = 2
LANES = 128
MESH = pl.DeviceIdType.MESH
F32 = jnp.float32
BF16 = jnp.bfloat16


def two_pieces(x):
    high = x.astype(BF16)
    low = (x - high.astype(F32)).astype(BF16)
    return high, low


def swap_groups(x, slots):
    height, lanes = x.shape
    row = lax.broadcasted_iota(jnp.int32, x.shape, 0)
    lane = lax.broadcasted_iota(jnp.int32, x.shape, 1)
    bit = 1
    while bit < height:
        step = bit * slots
        differ = ((row * slots) ^ lane) & step
        up = pltpu.roll(pltpu.roll(x, bit, 0), lanes - step, 1)
        down = pltpu.roll(pltpu.roll(x, height - bit, 0), step, 1)
        x = jnp.where(differ == 0, x, jnp.where((row & bit) != 0, up, down))
        bit *= 2
    return x


def wait_bytes(ref, sem):
    pltpu.make_async_copy(ref, ref, sem).wait()


def kernel(
    n,
    rhs_h,
    psi_h,
    dinv_h,
    jac_h,
    rec_h,
    don_h,
    wgt_h,
    live_h,
    out_ref,
    total_ref,
    rhs,
    psi0,
    psi1,
    dinv,
    jac,
    rec,
    don,
    wgt,
    live_s,
    acc,
    near,
    recpad,
    stage,
    first_out,
    first_in,
    later_out,
    later_in,
    hsend,
    hrecv,
    nsend,
    nrecv,
    pick_hot,
    pick_block,
    add_hot,
    add_block,
    lhs,
    weights,
    local_sem,
    v_sem,
    h_sem,
    n_sem,
):
    nvar, rows, cols = psi0.shape
    slots = rec.shape[1]
    donors = don.shape[1]
    lists = n * slots
    per = LANES // slots
    tiles = lists // LANES
    width = pick_hot.shape[0]
    strips = cols // width
    blocks = rows * strips
    full = nvar * blocks
    me = lax.axis_index("blk")
    design = lax.axis_index("design")

    mirrored = me < n // 2
    place = jnp.where(mirrored, n - 1 - me, me)

    def partner(k):
        other = jnp.where(k >= place, k + 1, k)
        return jnp.where(mirrored, n - 1 - other, other)

    barrier = pltpu.get_barrier_semaphore()

    def greet(k, carry):
        pl.semaphore_signal(
            barrier, inc=1, device_id=(design, partner(k)), device_id_type=MESH
        )
        return carry

    lax.fori_loop(0, n - 1, greet, 0)

    loads = []
    for k, (src, dst) in enumerate(
        (
            (rec_h.at[0], rec),
            (don_h.at[0], don),
            (wgt_h.at[0], wgt),
            (psi_h, psi0),
            (jac_h, jac),
            (rhs_h, rhs),
            (dinv_h, dinv),
            (live_h, live_s),
        )
    ):
        copy = pltpu.make_async_copy(src, dst, local_sem.at[k])
        copy.start()
        loads.append(copy)

    def split_cell(row):
        i = jnp.floor((row + 0.5) * (1.0 / cols))
        j = row - i * cols
        q = jnp.floor((j + 0.5) * (1.0 / width))
        return (q * rows + i).astype(jnp.int32), (j - q * width).astype(jnp.int32)

    def to_all(source_of, dest_ref, send_sem, recv_sem):
        def send(k, carry):
            dest = partner(k)
            pltpu.make_async_remote_copy(
                src_ref=source_of(dest),
                dst_ref=dest_ref.at[me],
                send_sem=send_sem,
                recv_sem=recv_sem,
                device_id=(design, dest),
                device_id_type=MESH,
            ).start()
            return carry

        lax.fori_loop(0, n - 1, send, 0)

    def halo_copies(sweep):
        below = lax.rem(me + n - 1, n)
        above = lax.rem(me + 1, n)
        return [
            pltpu.make_async_remote_copy(
                src_ref=hsend.at[sweep, side],
                dst_ref=hrecv.at[sweep, side],
                send_sem=h_sem.at[sweep, 0],
                recv_sem=h_sem.at[sweep, 1],
                device_id=(design, target),
                device_id_type=MESH,
            )
            for side, target in ((0, above), (1, below))
        ]

    def assemble(tile_of):
        parts = []
        for h in range(tiles):
            total = None
            for g in range(per):
                tile = tile_of(h * per + g)
                if g:
                    tile = pltpu.roll(tile, g * slots, 1)
                total = tile if total is None else total + tile
            parts.append(total)
        return parts

    def put_halo(sweep, psi):
        hsend[sweep, 0] = psi[:, rows - 1, :]
        hsend[sweep, 1] = psi[:, 0, :]

    def pick(sweep, psi):
        x = jnp.concatenate(
            [psi[a, :, q * width : (q + 1) * width] for a in range(nvar) for q in range(strips)],
            axis=0,
        )
        high, low = two_pieces(x)
        got = jnp.dot(
            jnp.concatenate([high, low], axis=0), pick_hot[...], preferred_element_type=F32
        )
        got = (got[:full] + got[full:]).reshape(nvar, blocks, lists)
        got = jnp.sum(got * pick_block[...][None], axis=1)
        got = jnp.concatenate([got, jnp.zeros((per - nvar, lists), F32)], axis=0)
        for h in range(tiles):
            packed = swap_groups(got[:, h * LANES : (h + 1) * LANES], slots)
            if sweep == 0:
                first_out[h * per : (h + 1) * per, 1, :] = packed
            else:
                later_out[sweep - 1, h * per : (h + 1) * per, 0, :] = packed

    stage[...] = jnp.zeros(stage.shape, F32)
    recpad[...] = jnp.zeros(recpad.shape, F32)
    loads[0].wait()
    recpad[:, 0:slots] = rec[...].astype(F32)
    cells = jnp.concatenate(assemble(lambda d: recpad[d : d + 1, :]), axis=1)
    upper, lower = split_cell(cells)
    pick_hot[...] = (
        lax.broadcasted_iota(jnp.int32, (width, lists), 0) == lower
    ).astype(F32).astype(BF16)
    pick_block[...] = (lax.broadcasted_iota(jnp.int32, (blocks, lists), 0) == upper).astype(F32)
    loads[1].wait()
    loads[2].wait()
    loads[7].wait()
    slot_id = lax.broadcasted_iota(jnp.int32, (donors, slots), 1)
    for d in range(n):
        stage[d, 0:donors, 0:slots] = don[d].astype(F32)
        stage[d, donors : 2 * donors, 0:slots] = jnp.where(slot_id < live_s[0, d], wgt[d], 0.0)
    for h, part in enumerate(assemble(lambda d: stage[d])):
        first_out[h * per : (h + 1) * per, 0, :] = swap_groups(part, slots)
    loads[3].wait()
    put_halo(0, psi0)
    pick(0, psi0)

    pl.semaphore_wait(barrier, n - 1)
    halos = [halo_copies(s) for s in range(SWEEPS)]
    to_all(lambda dest: first_out.at[dest], first_in, v_sem.at[0, 0], v_sem.at[0, 1])
    for copy in halos[0]:
        copy.start()

    def couple(psi, sweep, faces, first):
        def chunk(c, carry):
            at = pl.ds(pl.multiple_of(c * LANES, LANES), LANES)
            values = [[near[f, b, :, at] for b in range(nvar)] for f in faces]
            for a in range(nvar):
                total = rhs[a, :, at] if first else acc[a, :, at]
                for k, f in enumerate(faces):
                    for b in range(nvar):
                        total = total - jac[f, a, b, :, at].astype(F32) * values[k][b]
                acc[a, :, at] = total
            return carry

        lax.fori_loop(0, cols // LANES, chunk, 0, unroll=2)

    col_id = lax.broadcasted_iota(jnp.int32, (rows, cols), 1)
    row_id = lax.broadcasted_iota(jnp.int32, (rows, cols), 0)

    def sides(psi, sweep):
        for b in range(nvar):
            x = psi[b]
            near[2, b] = jnp.where(col_id == 0, 0.0, pltpu.roll(x, 1, 1))
            near[3, b] = jnp.where(col_id == cols - 1, 0.0, pltpu.roll(x, cols - 1, 1))

    def ends(psi, sweep):
        wait_bytes(hrecv.at[sweep], h_sem.at[sweep, 1])
        for b in range(nvar):
            x = psi[b]
            low = jnp.where(me > 0, hrecv[sweep, 0, b : b + 1, :], 0.0)
            high = jnp.where(me < n - 1, hrecv[sweep, 1, b : b + 1, :], 0.0)
            near[0, b] = jnp.where(row_id == 0, low, pltpu.roll(x, 1, 0))
            near[1, b] = jnp.where(row_id == rows - 1, high, pltpu.roll(x, rows - 1, 0))

    def prepare_adds():
        wait_bytes(first_in.at[pl.ds(0, n - 1)], v_sem.at[0, 1])
        first_in[me] = first_out[me]
        packed = jnp.concatenate(
            [
                swap_groups(first_in[h * per : (h + 1) * per, 0, :], slots)
                for h in range(tiles)
            ],
            axis=1,
        )
        weights[...] = packed[donors : 2 * donors]
        for m in range(donors):
            upper, lower = split_cell(packed[m : m + 1])
            at = slice(m * lists, (m + 1) * lists)
            add_hot[:, at] = (
                lax.broadcasted_iota(jnp.int32, (width, lists), 0) == lower
            ).astype(F32).astype(BF16)
            add_block[m] = (
                lax.broadcasted_iota(jnp.int32, (blocks, lists), 0) == upper
            ).astype(F32)

    def add_donors(sweep):
        if sweep == 0:
            parts = [first_in[h * per : (h + 1) * per, 1, :] for h in range(tiles)]
        else:
            wait_bytes(later_in.at[sweep - 1, pl.ds(0, n - 1)], v_sem.at[sweep, 1])
            later_in[sweep - 1, me] = later_out[sweep - 1, me]
            parts = [
                later_in[sweep - 1, h * per : (h + 1) * per, 0, :] for h in range(tiles)
            ]
        values = jnp.concatenate([swap_groups(part, slots) for part in parts], axis=1)
        for m in range(donors):
            terms = values * weights[m : m + 1, :]
            pieces = two_pieces(terms)
            for k, piece in enumerate(pieces):
                piece = piece.astype(F32)
                for a in range(nvar):
                    at = k * full + a * blocks
                    lhs[at : at + blocks, m * lists : (m + 1) * lists] = (
                        add_block[m] * piece[a : a + 1, :]
                    ).astype(BF16)
        got = lax.dot_general(
            lhs[...], add_hot[...], (((1,), (1,)), ((), ())), preferred_element_type=F32
        )
        got = got[:full] + got[full:]
        for a in range(nvar):
            for q in range(strips):
                at = a * blocks + q * rows
                col = slice(q * width, (q + 1) * width)
                acc[a, :, col] = acc[a, :, col] + got[at : at + rows]

    def finish(psi, new):
        def chunk(c, total):
            at = pl.ds(pl.multiple_of(c * LANES, LANES), LANES)
            source = [acc[b, :, at] for b in range(nvar)]
            for a in range(nvar):
                value = dinv[a, 0, :, at] * source[0]
                for b in range(1, nvar):
                    value = value + dinv[a, b, :, at] * source[b]
                change = value - psi[a, :, at]
                total = total + change * change
                new[a, :, at] = value
            return total

        return lax.fori_loop(0, cols // LANES, chunk, jnp.zeros((rows, LANES), F32), unroll=2)

    sums = []
    psi = psi0
    for sweep in range(SWEEPS):
        new = out_ref if sweep == SWEEPS - 1 else psi1
        sides(psi, sweep)
        if sweep == 0:
            loads[4].wait()
            loads[5].wait()
        couple(psi, sweep, (2, 3), True)
        if sweep == 0:
            def square(c, total):
                at = pl.ds(pl.multiple_of(c * LANES, LANES), LANES)
                for a in range(nvar):
                    value = rhs[a, :, at]
                    total = total + value * value
                return total

            sums.append(
                lax.fori_loop(0, cols // LANES, square, jnp.zeros((rows, LANES), F32), unroll=2)
            )
        ends(psi, sweep)
        couple(psi, sweep, (0, 1), False)
        if sweep == 0:
            prepare_adds()
        add_donors(sweep)
        if sweep == 0:
            loads[6].wait()
        sums.append(finish(psi, new))
        psi = new
        if sweep + 1 < SWEEPS:
            pick(sweep + 1, psi)
            to_all(
                lambda dest: later_out.at[sweep, dest],
                later_in.at[sweep],
                v_sem.at[sweep + 1, 0],
                v_sem.at[sweep + 1, 1],
            )
            put_halo(sweep + 1, psi)
            for copy in halos[sweep + 1]:
                copy.start()

    lane = lax.broadcasted_iota(jnp.int32, (1, LANES), 1)
    row = jnp.zeros((1, LANES), F32)
    for q, part in enumerate(sums):
        line = jnp.sum(part, axis=0, keepdims=True)
        line = line + pltpu.roll(line, 64, 1)
        line = line + pltpu.roll(line, 32, 1)
        row = jnp.where((lane >= 32 * q) & (lane < 32 * (q + 1)), line, row)
    nsend[...] = row
    to_all(lambda dest: nsend, nrecv, n_sem.at[0], n_sem.at[1])
    wait_bytes(first_in.at[pl.ds(0, n - 1)], v_sem.at[0, 0])
    for sweep in range(SWEEPS):
        if sweep:
            wait_bytes(later_in.at[sweep - 1, pl.ds(0, n - 1)], v_sem.at[sweep, 0])
        wait_bytes(hsend.at[sweep], h_sem.at[sweep, 0])
    wait_bytes(nrecv.at[pl.ds(0, n - 1)], n_sem.at[1])
    nrecv[me] = nsend[...]
    total = nrecv[0]
    for s in range(1, n):
        total = total + nrecv[s]
    total_ref[...] = total
    wait_bytes(nrecv.at[pl.ds(0, n - 1)], n_sem.at[0])


def close(adjoint_ref, total_ref, out_h, norm_h, norm_s, sem):
    copy = pltpu.make_async_copy(adjoint_ref, out_h, sem.at[0])
    copy.start()
    lane = lax.broadcasted_iota(jnp.int32, (1, LANES), 1)
    total = total_ref[...]
    sums = [
        jnp.sum(
            jnp.where((lane >= 32 * q) & (lane < 32 * (q + 1)), total, 0.0), axis=1, keepdims=True
        )
        for q in range(SWEEPS + 1)
    ]
    for k in range(SWEEPS):
        result = jnp.sqrt(sums[k + 1] / (sums[0] + 1e-6))
        norm_s[k] = result[0, 0]
    last = pltpu.make_async_copy(norm_s, norm_h, sem.at[1])
    last.start()
    copy.wait()
    last.wait()


def body(n, right_side, adjoint_start, diag_inverse, face_jacobian, receptor, donor, weight, live):
    nvar, rows, cols = right_side.shape
    slots = receptor.shape[2]
    donors = donor.shape[2]
    lists = n * slots
    width = min(256, cols)
    blocks = rows * (cols // width)
    any_space = pl.BlockSpec(memory_space=pl.ANY)
    field = pltpu.VMEM((nvar, rows, cols), F32)
    placed = [
        pltpu.with_memory_space_constraint(x, pltpu.HBM)
        for x in (
            right_side,
            adjoint_start,
            diag_inverse,
            face_jacobian,
            receptor,
            donor,
            weight,
            live,
        )
    ]
    adjoint, total = pl.pallas_call(
        functools.partial(kernel, n),
        out_shape=(
            jax.ShapeDtypeStruct((nvar, rows, cols), F32),
            jax.ShapeDtypeStruct((1, LANES), F32),
        ),
        in_specs=[pl.BlockSpec(memory_space=pltpu.HBM)] * 8,
        out_specs=(
            pl.BlockSpec(memory_space=pltpu.VMEM),
            pl.BlockSpec(memory_space=pltpu.VMEM),
        ),
        scratch_shapes=[
            field,
            field,
            field,
            pltpu.VMEM(diag_inverse.shape, F32),
            pltpu.VMEM(face_jacobian.shape, face_jacobian.dtype),
            pltpu.VMEM((n, slots), jnp.int32),
            pltpu.VMEM((n, donors, slots), jnp.int32),
            pltpu.VMEM((n, donors, slots), F32),
            pltpu.SMEM((1, n), jnp.int32),
            field,
            pltpu.VMEM((4, nvar, rows, cols), F32),
            pltpu.VMEM((n, LANES), F32),
            pltpu.VMEM((n, 2 * donors, LANES), F32),
            pltpu.VMEM((n, 2, LANES), F32),
            pltpu.VMEM((n, 2, LANES), F32),
            pltpu.VMEM((SWEEPS - 1, n, 1, LANES), F32),
            pltpu.VMEM((SWEEPS - 1, n, 1, LANES), F32),
            pltpu.VMEM((SWEEPS, 2, nvar, cols), F32),
            pltpu.VMEM((SWEEPS, 2, nvar, cols), F32),
            pltpu.VMEM((1, LANES), F32),
            pltpu.VMEM((n, 1, LANES), F32),
            pltpu.VMEM((width, lists), BF16),
            pltpu.VMEM((blocks, lists), F32),
            pltpu.VMEM((width, donors * lists), BF16),
            pltpu.VMEM((donors, blocks, lists), F32),
            pltpu.VMEM((2 * nvar * blocks, donors * lists), BF16),
            pltpu.VMEM((donors, lists), F32),
            pltpu.SemaphoreType.DMA((8,)),
            pltpu.SemaphoreType.DMA((SWEEPS, 2)),
            pltpu.SemaphoreType.DMA((SWEEPS, 2)),
            pltpu.SemaphoreType.DMA((2,)),
        ],
        compiler_params=pltpu.CompilerParams(
            collective_id=0, has_side_effects=True, vmem_limit_bytes=36 * 1024 * 1024
        ),
    )(*placed)
    return pl.pallas_call(
        close,
        out_shape=(
            jax.ShapeDtypeStruct((nvar, rows, cols), F32),
            jax.ShapeDtypeStruct((SWEEPS,), F32),
        ),
        in_specs=[pl.BlockSpec(memory_space=pltpu.VMEM)] * 2,
        out_specs=(any_space, any_space),
        scratch_shapes=[pltpu.SMEM((SWEEPS,), F32), pltpu.SemaphoreType.DMA((2,))],
        compiler_params=pltpu.CompilerParams(vmem_limit_bytes=8 * 1024 * 1024),
    )(adjoint, total)


def solution(mesh):
    return jax.shard_map(
        functools.partial(body, mesh.shape["blk"]),
        mesh=mesh,
        in_specs=(
            P(None, ("design", "blk"), None),
            P(None, ("design", "blk"), None),
            P(None, None, ("design", "blk"), None),
            P(None, None, None, ("design", "blk"), None),
            P(("design", "blk"), None, None),
            P(("design", "blk"), None, None, None),
            P(("design", "blk"), None, None, None),
            P(("design", "blk"), None),
        ),
        out_specs=(P(None, ("design", "blk"), None), P("design")),
        check_vma=False,
    )
```

```python
import functools

import jax
import jax.numpy as jnp
from jax import lax
from jax.experimental import pallas as pl
from jax.experimental.pallas import tpu as pltpu
from jax.sharding import PartitionSpec as P

SWEEPS = 2
LANES = 128
MESH = pl.DeviceIdType.MESH
F32 = jnp.float32
BF16 = jnp.bfloat16


def two_pieces(x):
    high = x.astype(BF16)
    low = (x - high.astype(F32)).astype(BF16)
    return high, low


def swap_groups(x, slots):
    height, lanes = x.shape
    row = lax.broadcasted_iota(jnp.int32, x.shape, 0)
    lane = lax.broadcasted_iota(jnp.int32, x.shape, 1)
    bit = 1
    while bit < height:
        step = bit * slots
        differ = ((row * slots) ^ lane) & step
        up = pltpu.roll(pltpu.roll(x, bit, 0), lanes - step, 1)
        down = pltpu.roll(pltpu.roll(x, height - bit, 0), step, 1)
        x = jnp.where(differ == 0, x, jnp.where((row & bit) != 0, up, down))
        bit *= 2
    return x


def wait_bytes(ref, sem):
    pltpu.make_async_copy(ref, ref, sem).wait()


def kernel(
    n,
    rhs_h,
    psi_h,
    dinv_h,
    jac_h,
    rec_h,
    don_h,
    wgt_h,
    live_h,
    out_ref,
    total_ref,
    rhs,
    psi0,
    psi1,
    dinv,
    jac,
    rec,
    don,
    wgt,
    live_s,
    acc,
    near,
    recpad,
    stage,
    first_out,
    first_in,
    later_out,
    later_in,
    hsend,
    hrecv,
    nsend,
    nrecv,
    pick_hot,
    pick_block,
    add_hot,
    add_block,
    lhs,
    weights,
    local_sem,
    v_sem,
    h_sem,
    n_sem,
):
    nvar, rows, cols = psi0.shape
    slots = rec.shape[1]
    donors = don.shape[1]
    lists = n * slots
    per = LANES // slots
    tiles = lists // LANES
    width = pick_hot.shape[0]
    strips = cols // width
    blocks = rows * strips
    full = nvar * blocks
    me = lax.axis_index("blk")
    design = lax.axis_index("design")

    mirrored = me < n // 2
    place = jnp.where(mirrored, n - 1 - me, me)

    def partner(k):
        other = jnp.where(k >= place, k + 1, k)
        return jnp.where(mirrored, n - 1 - other, other)

    barrier = pltpu.get_barrier_semaphore()

    def greet(k, carry):
        pl.semaphore_signal(
            barrier, inc=1, device_id=(design, partner(k)), device_id_type=MESH
        )
        return carry

    lax.fori_loop(0, n - 1, greet, 0)

    loads = []
    for k, (src, dst) in enumerate(
        (
            (rec_h.at[0], rec),
            (don_h.at[0], don),
            (wgt_h.at[0], wgt),
            (psi_h, psi0),
            (jac_h, jac),
            (rhs_h, rhs),
            (dinv_h, dinv),
            (live_h, live_s),
        )
    ):
        copy = pltpu.make_async_copy(src, dst, local_sem.at[k])
        copy.start()
        loads.append(copy)

    def split_cell(row):
        i = jnp.floor((row + 0.5) * (1.0 / cols))
        j = row - i * cols
        q = jnp.floor((j + 0.5) * (1.0 / width))
        return (q * rows + i).astype(jnp.int32), (j - q * width).astype(jnp.int32)

    def to_all(source_of, dest_ref, send_sem, recv_sem):
        def send(k, carry):
            dest = partner(k)
            pltpu.make_async_remote_copy(
                src_ref=source_of(dest),
                dst_ref=dest_ref.at[me],
                send_sem=send_sem,
                recv_sem=recv_sem,
                device_id=(design, dest),
                device_id_type=MESH,
            ).start()
            return carry

        lax.fori_loop(0, n - 1, send, 0)

    def halo_copies(sweep):
        below = lax.rem(me + n - 1, n)
        above = lax.rem(me + 1, n)
        return [
            pltpu.make_async_remote_copy(
                src_ref=hsend.at[sweep, side],
                dst_ref=hrecv.at[sweep, side],
                send_sem=h_sem.at[sweep, 0],
                recv_sem=h_sem.at[sweep, 1],
                device_id=(design, target),
                device_id_type=MESH,
            )
            for side, target in ((0, above), (1, below))
        ]

    def assemble(tile_of):
        parts = []
        for h in range(tiles):
            total = None
            for g in range(per):
                tile = tile_of(h * per + g)
                if g:
                    tile = pltpu.roll(tile, g * slots, 1)
                total = tile if total is None else total + tile
            parts.append(total)
        return parts

    def put_halo(sweep, psi):
        hsend[sweep, 0] = psi[:, rows - 1, :]
        hsend[sweep, 1] = psi[:, 0, :]

    def pick(sweep, psi):
        x = jnp.concatenate(
            [psi[a, :, q * width : (q + 1) * width] for a in range(nvar) for q in range(strips)],
            axis=0,
        )
        high, low = two_pieces(x)
        got = jnp.dot(
            jnp.concatenate([high, low], axis=0), pick_hot[...], preferred_element_type=F32
        )
        got = (got[:full] + got[full:]).reshape(nvar, blocks, lists)
        got = jnp.sum(got * pick_block[...][None], axis=1)
        got = jnp.concatenate([got, jnp.zeros((per - nvar, lists), F32)], axis=0)
        for h in range(tiles):
            packed = swap_groups(got[:, h * LANES : (h + 1) * LANES], slots)
            if sweep == 0:
                first_out[h * per : (h + 1) * per, 1, :] = packed
            else:
                later_out[sweep - 1, h * per : (h + 1) * per, 0, :] = packed

    stage[...] = jnp.zeros(stage.shape, F32)
    recpad[...] = jnp.zeros(recpad.shape, F32)
    loads[0].wait()
    recpad[:, 0:slots] = rec[...].astype(F32)
    cells = jnp.concatenate(assemble(lambda d: recpad[d : d + 1, :]), axis=1)
    upper, lower = split_cell(cells)
    pick_hot[...] = (
        lax.broadcasted_iota(jnp.int32, (width, lists), 0) == lower
    ).astype(F32).astype(BF16)
    pick_block[...] = (lax.broadcasted_iota(jnp.int32, (blocks, lists), 0) == upper).astype(F32)
    loads[1].wait()
    loads[2].wait()
    loads[7].wait()
    slot_id = lax.broadcasted_iota(jnp.int32, (donors, slots), 1)
    for d in range(n):
        stage[d, 0:donors, 0:slots] = don[d].astype(F32)
        stage[d, donors : 2 * donors, 0:slots] = jnp.where(slot_id < live_s[0, d], wgt[d], 0.0)
    for h, part in enumerate(assemble(lambda d: stage[d])):
        first_out[h * per : (h + 1) * per, 0, :] = swap_groups(part, slots)
    loads[3].wait()
    put_halo(0, psi0)
    pick(0, psi0)

    pl.semaphore_wait(barrier, n - 1)
    halos = [halo_copies(s) for s in range(SWEEPS)]
    to_all(lambda dest: first_out.at[dest], first_in, v_sem.at[0, 0], v_sem.at[0, 1])
    for copy in halos[0]:
        copy.start()

    def couple(psi, sweep, faces, first):
        def chunk(c, carry):
            at = pl.ds(pl.multiple_of(c * LANES, LANES), LANES)
            values = [[near[f, b, :, at] for b in range(nvar)] for f in faces]
            for a in range(nvar):
                total = rhs[a, :, at] if first else acc[a, :, at]
                for k, f in enumerate(faces):
                    for b in range(nvar):
                        total = total - jac[f, a, b, :, at].astype(F32) * values[k][b]
                acc[a, :, at] = total
            return carry

        lax.fori_loop(0, cols // LANES, chunk, 0, unroll=2)

    col_id = lax.broadcasted_iota(jnp.int32, (rows, cols), 1)
    row_id = lax.broadcasted_iota(jnp.int32, (rows, cols), 0)

    def sides(psi, sweep):
        for b in range(nvar):
            x = psi[b]
            near[2, b] = jnp.where(col_id == 0, 0.0, pltpu.roll(x, 1, 1))
            near[3, b] = jnp.where(col_id == cols - 1, 0.0, pltpu.roll(x, cols - 1, 1))

    def ends(psi, sweep):
        wait_bytes(hrecv.at[sweep], h_sem.at[sweep, 1])
        for b in range(nvar):
            x = psi[b]
            low = jnp.where(me > 0, hrecv[sweep, 0, b : b + 1, :], 0.0)
            high = jnp.where(me < n - 1, hrecv[sweep, 1, b : b + 1, :], 0.0)
            near[0, b] = jnp.where(row_id == 0, low, pltpu.roll(x, 1, 0))
            near[1, b] = jnp.where(row_id == rows - 1, high, pltpu.roll(x, rows - 1, 0))

    def prepare_adds():
        wait_bytes(first_in.at[pl.ds(0, n - 1)], v_sem.at[0, 1])
        first_in[me] = first_out[me]
        packed = jnp.concatenate(
            [
                swap_groups(first_in[h * per : (h + 1) * per, 0, :], slots)
                for h in range(tiles)
            ],
            axis=1,
        )
        weights[...] = packed[donors : 2 * donors]
        for m in range(donors):
            upper, lower = split_cell(packed[m : m + 1])
            at = slice(m * lists, (m + 1) * lists)
            add_hot[:, at] = (
                lax.broadcasted_iota(jnp.int32, (width, lists), 0) == lower
            ).astype(F32).astype(BF16)
            add_block[m] = (
                lax.broadcasted_iota(jnp.int32, (blocks, lists), 0) == upper
            ).astype(F32)

    def add_donors(sweep):
        if sweep == 0:
            parts = [first_in[h * per : (h + 1) * per, 1, :] for h in range(tiles)]
        else:
            wait_bytes(later_in.at[sweep - 1, pl.ds(0, n - 1)], v_sem.at[sweep, 1])
            later_in[sweep - 1, me] = later_out[sweep - 1, me]
            parts = [
                later_in[sweep - 1, h * per : (h + 1) * per, 0, :] for h in range(tiles)
            ]
        values = jnp.concatenate([swap_groups(part, slots) for part in parts], axis=1)
        for m in range(donors):
            terms = values * weights[m : m + 1, :]
            pieces = two_pieces(terms)
            for k, piece in enumerate(pieces):
                piece = piece.astype(F32)
                for a in range(nvar):
                    at = k * full + a * blocks
                    lhs[at : at + blocks, m * lists : (m + 1) * lists] = (
                        add_block[m] * piece[a : a + 1, :]
                    ).astype(BF16)
        got = lax.dot_general(
            lhs[...], add_hot[...], (((1,), (1,)), ((), ())), preferred_element_type=F32
        )
        got = got[:full] + got[full:]
        for a in range(nvar):
            for q in range(strips):
                at = a * blocks + q * rows
                col = slice(q * width, (q + 1) * width)
                acc[a, :, col] = acc[a, :, col] + got[at : at + rows]

    def finish(psi, new):
        def chunk(c, total):
            at = pl.ds(pl.multiple_of(c * LANES, LANES), LANES)
            source = [acc[b, :, at] for b in range(nvar)]
            for a in range(nvar):
                value = dinv[a, 0, :, at] * source[0]
                for b in range(1, nvar):
                    value = value + dinv[a, b, :, at] * source[b]
                change = value - psi[a, :, at]
                total = total + change * change
                new[a, :, at] = value
            return total

        return lax.fori_loop(0, cols // LANES, chunk, jnp.zeros((rows, LANES), F32), unroll=True)

    sums = []
    psi = psi0
    for sweep in range(SWEEPS):
        new = out_ref if sweep == SWEEPS - 1 else psi1
        sides(psi, sweep)
        if sweep == 0:
            loads[4].wait()
            loads[5].wait()
        couple(psi, sweep, (2, 3), True)
        if sweep == 0:
            def square(c, total):
                at = pl.ds(pl.multiple_of(c * LANES, LANES), LANES)
                for a in range(nvar):
                    value = rhs[a, :, at]
                    total = total + value * value
                return total

            sums.append(
                lax.fori_loop(0, cols // LANES, square, jnp.zeros((rows, LANES), F32), unroll=2)
            )
        ends(psi, sweep)
        couple(psi, sweep, (0, 1), False)
        if sweep == 0:
            prepare_adds()
        add_donors(sweep)
        if sweep == 0:
            loads[6].wait()
        sums.append(finish(psi, new))
        psi = new
        if sweep + 1 < SWEEPS:
            pick(sweep + 1, psi)
            to_all(
                lambda dest: later_out.at[sweep, dest],
                later_in.at[sweep],
                v_sem.at[sweep + 1, 0],
                v_sem.at[sweep + 1, 1],
            )
            put_halo(sweep + 1, psi)
            for copy in halos[sweep + 1]:
                copy.start()

    lane = lax.broadcasted_iota(jnp.int32, (1, LANES), 1)
    row = jnp.zeros((1, LANES), F32)
    for q, part in enumerate(sums):
        line = jnp.sum(part, axis=0, keepdims=True)
        line = line + pltpu.roll(line, 64, 1)
        line = line + pltpu.roll(line, 32, 1)
        row = jnp.where((lane >= 32 * q) & (lane < 32 * (q + 1)), line, row)
    nsend[...] = row
    to_all(lambda dest: nsend, nrecv, n_sem.at[0], n_sem.at[1])
    wait_bytes(first_in.at[pl.ds(0, n - 1)], v_sem.at[0, 0])
    for sweep in range(SWEEPS):
        if sweep:
            wait_bytes(later_in.at[sweep - 1, pl.ds(0, n - 1)], v_sem.at[sweep, 0])
        wait_bytes(hsend.at[sweep], h_sem.at[sweep, 0])
    wait_bytes(nrecv.at[pl.ds(0, n - 1)], n_sem.at[1])
    nrecv[me] = nsend[...]
    total = nrecv[0]
    for s in range(1, n):
        total = total + nrecv[s]
    total_ref[...] = total
    wait_bytes(nrecv.at[pl.ds(0, n - 1)], n_sem.at[0])


def close(adjoint_ref, total_ref, out_h, norm_h, norm_s, sem):
    copy = pltpu.make_async_copy(adjoint_ref, out_h, sem.at[0])
    copy.start()
    lane = lax.broadcasted_iota(jnp.int32, (1, LANES), 1)
    total = total_ref[...]
    sums = [
        jnp.sum(
            jnp.where((lane >= 32 * q) & (lane < 32 * (q + 1)), total, 0.0), axis=1, keepdims=True
        )
        for q in range(SWEEPS + 1)
    ]
    for k in range(SWEEPS):
        result = jnp.sqrt(sums[k + 1] / (sums[0] + 1e-6))
        norm_s[k] = result[0, 0]
    last = pltpu.make_async_copy(norm_s, norm_h, sem.at[1])
    last.start()
    copy.wait()
    last.wait()


def body(n, right_side, adjoint_start, diag_inverse, face_jacobian, receptor, donor, weight, live):
    nvar, rows, cols = right_side.shape
    slots = receptor.shape[2]
    donors = donor.shape[2]
    lists = n * slots
    width = min(256, cols)
    blocks = rows * (cols // width)
    any_space = pl.BlockSpec(memory_space=pl.ANY)
    field = pltpu.VMEM((nvar, rows, cols), F32)
    placed = [
        pltpu.with_memory_space_constraint(x, pltpu.HBM)
        for x in (
            right_side,
            adjoint_start,
            diag_inverse,
            face_jacobian,
            receptor,
            donor,
            weight,
            live,
        )
    ]
    adjoint, total = pl.pallas_call(
        functools.partial(kernel, n),
        out_shape=(
            jax.ShapeDtypeStruct((nvar, rows, cols), F32),
            jax.ShapeDtypeStruct((1, LANES), F32),
        ),
        in_specs=[pl.BlockSpec(memory_space=pltpu.HBM)] * 8,
        out_specs=(
            pl.BlockSpec(memory_space=pltpu.VMEM),
            pl.BlockSpec(memory_space=pltpu.VMEM),
        ),
        scratch_shapes=[
            field,
            field,
            field,
            pltpu.VMEM(diag_inverse.shape, F32),
            pltpu.VMEM(face_jacobian.shape, face_jacobian.dtype),
            pltpu.VMEM((n, slots), jnp.int32),
            pltpu.VMEM((n, donors, slots), jnp.int32),
            pltpu.VMEM((n, donors, slots), F32),
            pltpu.SMEM((1, n), jnp.int32),
            field,
            pltpu.VMEM((4, nvar, rows, cols), F32),
            pltpu.VMEM((n, LANES), F32),
            pltpu.VMEM((n, 2 * donors, LANES), F32),
            pltpu.VMEM((n, 2, LANES), F32),
            pltpu.VMEM((n, 2, LANES), F32),
            pltpu.VMEM((SWEEPS - 1, n, 1, LANES), F32),
            pltpu.VMEM((SWEEPS - 1, n, 1, LANES), F32),
            pltpu.VMEM((SWEEPS, 2, nvar, cols), F32),
            pltpu.VMEM((SWEEPS, 2, nvar, cols), F32),
            pltpu.VMEM((1, LANES), F32),
            pltpu.VMEM((n, 1, LANES), F32),
            pltpu.VMEM((width, lists), BF16),
            pltpu.VMEM((blocks, lists), F32),
            pltpu.VMEM((width, donors * lists), BF16),
            pltpu.VMEM((donors, blocks, lists), F32),
            pltpu.VMEM((2 * nvar * blocks, donors * lists), BF16),
            pltpu.VMEM((donors, lists), F32),
            pltpu.SemaphoreType.DMA((8,)),
            pltpu.SemaphoreType.DMA((SWEEPS, 2)),
            pltpu.SemaphoreType.DMA((SWEEPS, 2)),
            pltpu.SemaphoreType.DMA((2,)),
        ],
        compiler_params=pltpu.CompilerParams(
            collective_id=0, has_side_effects=True, vmem_limit_bytes=36 * 1024 * 1024
        ),
    )(*placed)
    return pl.pallas_call(
        close,
        out_shape=(
            jax.ShapeDtypeStruct((nvar, rows, cols), F32),
            jax.ShapeDtypeStruct((SWEEPS,), F32),
        ),
        in_specs=[pl.BlockSpec(memory_space=pltpu.VMEM)] * 2,
        out_specs=(any_space, any_space),
        scratch_shapes=[pltpu.SMEM((SWEEPS,), F32), pltpu.SemaphoreType.DMA((2,))],
        compiler_params=pltpu.CompilerParams(vmem_limit_bytes=8 * 1024 * 1024),
    )(adjoint, total)


def solution(mesh):
    return jax.shard_map(
        functools.partial(body, mesh.shape["blk"]),
        mesh=mesh,
        in_specs=(
            P(None, ("design", "blk"), None),
            P(None, ("design", "blk"), None),
            P(None, None, ("design", "blk"), None),
            P(None, None, None, ("design", "blk"), None),
            P(("design", "blk"), None, None),
            P(("design", "blk"), None, None, None),
            P(("design", "blk"), None, None, None),
            P(("design", "blk"), None),
        ),
        out_specs=(P(None, ("design", "blk"), None), P("design")),
        check_vma=False,
    )
```
